256 devices in a mesh: kx: 16 (over z, x_lo), ky: 4 (over x_hi, core), kz: 4 (over y).
Axes of the slice: x: 4 (x_hi: 2, x_lo: 2; x = x_hi * 2 + x_lo), y: 4, z: 8, core: 2. Of those that a mesh axis runs over, the one named last changes fastest.
Arguments:
- coefficients: bfloat16 [2, 16, 4, 4, 512, 2048], P(None, 'kx', 'ky', 'kz'), may hold values from -1 to 1
- shift_blocks: int32 [3], replicated, may hold values from 1 to 15, as said below
Outputs:
- centre: float32 [3, 512], replicated
- spread: float32 [3, 512], replicated
- coherence: float32 [3, 16, 4, 4], P(None, 'kx', 'ky', 'kz')
The draws below stay inside these ranges and needn't reach their ends.
Inputs may be any that keep to these rules, and one draw needn't show every extreme that they name: The coefficients one period further along direction d are those of the first k-point of the string with plane-wave index g read at (g + 128 * shift_blocks[d]) mod 2048.
All inputs are finite; a program needn't handle non-finite values.
Results may differ from the reference program's by a relative error of at most 0.0003.
Values may be sent and summed in bfloat16 or wider, within the bound.
A program may use at most 128 MiB of HBM per device.

```python
import jax
import jax.numpy as jnp
from jax import lax

NB = 512
NGW = 2048
NX = 16
NY = 4
NZ = 4


def offsets_for(key):
    middle = jax.random.randint(jax.random.fold_in(key, 11), (1,), 1, NGW // 128).astype(jnp.int32)
    ends = jnp.array([1, NGW // 128 - 1], jnp.int32)
    values = jnp.concatenate([ends, middle])
    order = jax.random.permutation(jax.random.fold_in(key, 13), 3)
    return values[order].astype(jnp.int32)


def draw_shift_blocks(key, part):
    return offsets_for(key)


def mix_along(fields, shift, points, position):
    angles = jnp.arange(points, dtype=jnp.float32) * (jnp.pi / (2.0 * points))
    dims_shape = [1] * (fields.ndim + 1)
    dims_shape[position] = points
    cosine = jnp.cos(angles).reshape(dims_shape)
    sine = jnp.sin(angles).reshape(dims_shape)
    rolled = jnp.roll(fields, -shift, axis=-1)
    return cosine * jnp.expand_dims(fields, position) + sine * jnp.expand_dims(rolled, position)


def draw_coefficients(key, part):
    offsets = offsets_for(key) * 128
    subkeys = jax.random.split(jax.random.fold_in(key, 23), 5)
    entry_scale = 1.0 / jnp.sqrt(2.0 * NGW)
    common = jnp.clip(jax.random.normal(subkeys[0], (2, NB, NGW), jnp.float32), -6.0, 6.0) * entry_scale
    fields = mix_along(common, offsets[2], NZ, 1)
    fields = mix_along(fields, offsets[1], NY, 1)
    fields = mix_along(fields, offsets[0], NX, 1)
    full_shape = (2, NX, NY, NZ, NB, NGW)
    roughness = jnp.clip(jax.random.normal(subkeys[1], full_shape, jnp.float32), -6.0, 6.0)
    amplitude = jnp.exp(jax.random.uniform(subkeys[2], (NB,), jnp.float32, jnp.log(0.1), jnp.log(0.6)))
    jitter = 0.35
    fields = fields + amplitude[:, None] * roughness * entry_scale
    winding = jax.random.uniform(subkeys[3], (3, NB), jnp.float32, -0.2, 0.2)
    x_frac = jnp.arange(NX, dtype=jnp.float32) / NX
    y_frac = jnp.arange(NY, dtype=jnp.float32) / NY
    z_frac = jnp.arange(NZ, dtype=jnp.float32) / NZ
    angles = 2.0 * jnp.pi * (winding[0] * x_frac[:, None, None, None] + winding[1] * y_frac[None, :, None, None] + winding[2] * z_frac[None, None, :, None])
    angles = angles + jax.random.uniform(subkeys[4], (NX, NY, NZ, NB), jnp.float32, -jitter, jitter)
    cosine = jnp.cos(angles)[..., None]
    sine = jnp.sin(angles)[..., None]
    real_part = cosine * fields[0] - sine * fields[1]
    imag_part = sine * fields[0] + cosine * fields[1]
    return jnp.stack([real_part, imag_part]).astype(jnp.bfloat16)


def setup_inputs(seed: int = 0) -> dict:
    arg_keys = jax.random.split(jax.random.key(seed), 3)
    coefficients = draw_coefficients(jax.random.fold_in(arg_keys[2], 71), 0)
    shift_blocks = draw_shift_blocks(jax.random.fold_in(arg_keys[2], 71), 0)
    return dict(coefficients=coefficients, shift_blocks=shift_blocks)


def pair_measure(own_point, partner):
    bands = own_point.shape[1]
    left_side = jnp.concatenate([own_point[0], own_point[1]], axis=1)
    right_side = jnp.concatenate([jnp.concatenate([partner[0], partner[1]], axis=1), jnp.concatenate([partner[1], -partner[0]], axis=1)], axis=0)
    product = jnp.dot(left_side, right_side.T, preferred_element_type=jnp.float32)
    real_part = product[:, :bands]
    imag_part = product[:, bands:]
    phases = jnp.arctan2(jnp.diagonal(imag_part), jnp.diagonal(real_part))
    coherence = jnp.sum(real_part * real_part + imag_part * imag_part) / bands
    return phases, coherence


def reference(coefficients, shift_blocks):
    shifts = shift_blocks.astype(jnp.int32) * 128
    k_total = NX * NY * NZ
    counts = jnp.array([NX, NY, NZ], jnp.float32)

    def per_point(k_index):
        x_index = k_index // (NY * NZ)
        y_index = (k_index // NZ) % NY
        z_index = k_index % NZ
        own_point = coefficients[:, x_index, y_index, z_index]
        gathered_phases = []
        gathered_coherence = []
        for direction in range(3):
            coords = [x_index, y_index, z_index]
            limits = [NX, NY, NZ]
            wrapped = coords[direction] == limits[direction] - 1
            coords[direction] = (coords[direction] + 1) % limits[direction]
            partner = coefficients[:, coords[0], coords[1], coords[2]]
            partner = jnp.where(wrapped, jnp.roll(partner, -shifts[direction], axis=-1), partner)
            phases, coherence = pair_measure(own_point, partner)
            gathered_phases.append(phases)
            gathered_coherence.append(coherence)
        return jnp.stack(gathered_phases), jnp.stack(gathered_coherence)

    phases, coherence = lax.map(per_point, jnp.arange(k_total, dtype=jnp.int32))
    mean_phase = jnp.sum(phases, axis=0) / k_total
    deviation = phases - mean_phase[None]
    variance = jnp.sum(deviation * deviation, axis=0) / k_total
    centre = -counts[:, None] * mean_phase / (2.0 * jnp.pi)
    spread = (counts[:, None] / (2.0 * jnp.pi)) ** 2 * variance
    coherence_out = coherence.T.reshape(3, NX, NY, NZ)
    return centre, spread, coherence_out
```

```python
import functools

import jax
import jax.numpy as jnp
from jax import lax
from jax.experimental import pallas as pl
from jax.experimental.pallas import tpu as pltpu
from jax.sharding import PartitionSpec as P

SEND_ROWS = 32
STEP_ROWS = 64
HALF = 256
BLOCK = 128
TILE = 16
NT = (((1,), (1,)), ((), ()))


def kernel(
    nx, ny, nz,
    shift_ref, c_ref, out_ref, coh_ref,
    own, lhs1, lhs2, got, dre, dim, squares,
    plane, column, line,
    own_sem, send_a, send_y, send_fx, send_fz, recv,
    plane_send, plane_recv, column_send, column_recv, line_send, line_recv,
):
    kx, ky, kz = lax.axis_index("kx"), lax.axis_index("ky"), lax.axis_index("kz")
    bands, width = c_ref.shape[1], c_ref.shape[2]
    sends = bands // SEND_ROWS
    steps = bands // STEP_ROWS
    per_step = STEP_ROWS // SEND_ROWS
    half = min(HALF, bands)
    blocks = width // BLOCK
    levels = nx // 2
    xl, level = kx % 2, kx // 2
    core = ky % 2
    active = xl == core
    slot = xl * 4 + ky

    def device(x, y, z):
        return (x, y, z)

    def in_plane(index):
        return device(2 * level + index // 4, index % 4, kz)

    def in_column(index):
        return device(kx, ky, index)

    def in_line(index):
        return device(2 * index + xl, ky, kz)

    sibling = ky + 1 - 2 * core
    other_x = kx + 1 - 2 * xl
    up, down = (kz + 1) % nz, (kz + nz - 1) % nz

    barrier = pltpu.get_barrier_semaphore()
    peers = [in_plane((slot + step) % 8) for step in range(1, 8)]
    peers += [in_column((kz + step) % nz) for step in range(1, nz)]
    peers += [in_line((level + step) % levels) for step in range(1, levels)]
    peers += [device(kx, sibling, up), device(kx, sibling, down)]
    for peer in peers:
        pl.semaphore_signal(
            barrier, inc=1, device_id=peer, device_id_type=pl.DeviceIdType.MESH
        )
    load = pltpu.make_async_copy(c_ref, own, own_sem)
    load.start()
    pl.semaphore_wait(barrier, len(peers))

    def rows_of(index):
        return pl.ds(pl.multiple_of(index * SEND_ROWS, SEND_ROWS), SEND_ROWS)

    def remote(source, target_slot, index, send, target):
        return pltpu.make_async_remote_copy(
            src_ref=source.at[:, rows_of(index), :],
            dst_ref=got.at[target_slot, :, rows_of(index), :],
            send_sem=send.at[index],
            recv_sem=recv.at[target_slot, index],
            device_id=target,
            device_id_type=pl.DeviceIdType.MESH,
        )

    first_x = jnp.where(active, kx, other_x)
    first_y = jnp.where(active, sibling, ky)
    string_slot = jnp.where(active, 2, 1)
    string_y = jnp.where(active, sibling, ky)
    string_z = jnp.where(active, up, down)
    cross = device(other_x, 3 - ky, kz)
    along = device((kx + jnp.where(xl == 0, 2, nx - 2)) % nx, ky, kz)

    def to_first(index):
        return remote(c_ref, 0, index, send_a, device(first_x, first_y, kz))

    def to_string(index):
        return remote(c_ref, string_slot, index, send_y, device(kx, string_y, string_z))

    def to_cross(index):
        return remote(got.at[0], 2, index, send_fx, cross)

    def to_along(index):
        return remote(got.at[0], 1, index, send_fz, along)

    def arrived(edge, index):
        return pltpu.make_async_remote_copy(
            src_ref=got.at[edge, :, rows_of(index), :],
            dst_ref=got.at[edge, :, rows_of(index), :],
            send_sem=send_a.at[index],
            recv_sem=recv.at[edge, index],
            device_id=cross,
            device_id_type=pl.DeviceIdType.MESH,
        )

    def start_own(index, carry):
        to_first(index).start()
        to_string(index).start()
        return carry

    lax.fori_loop(0, sends, start_own, 0)

    dre[...] = jnp.zeros_like(dre)
    dim[...] = jnp.zeros_like(dim)
    squares[...] = jnp.zeros_like(squares)

    first_local = jnp.where(active, xl == 1, core == 1)
    second_local = jnp.logical_and(active, xl == 0)
    third_local = jnp.logical_or(jnp.logical_not(active), xl == 0)
    second_wrap = jnp.where(
        active, jnp.where(xl == 0, kx == 0, kx == nx - 1), kz == nz - 1
    )
    third_wrap = jnp.where(active, jnp.where(xl == 0, ky == 0, ky == ny - 1), kz == 0)
    chosen = active.astype(jnp.int32)
    second_shift = chosen * shift_ref[0] + (1 - chosen) * shift_ref[2]
    third_shift = chosen * shift_ref[1] + (1 - chosen) * shift_ref[2]

    def offset(shift, wrap, local):
        wrapped, kept = wrap.astype(jnp.int32), local.astype(jnp.int32)
        return wrapped * (kept * shift + (1 - kept) * (blocks - shift))

    second_offset = offset(second_shift, second_wrap, second_local)
    third_offset = offset(third_shift, third_wrap, third_local)

    def turn(source, target, amount):
        def body(tile, carry):
            rows = pl.ds(pl.multiple_of(tile * TILE, TILE), TILE)
            value = source[:, rows, :]
            reach = 1
            while reach < blocks:
                cut = reach * BLOCK
                moved = jnp.concatenate([value[:, :, cut:], value[:, :, :cut]], axis=2)
                value = jnp.where((amount // reach) % 2 == 1, moved, value)
                reach *= 2
            target[:, rows, :] = value
            return carry

        lax.fori_loop(0, bands // TILE, body, 0)

    load.wait()
    turn(own, lhs1, second_offset)

    @pl.when(active)
    def _():
        turn(own, lhs2, third_offset)

    @pl.when(jnp.logical_not(active))
    def _():
        def body(index, carry):
            arrived(0, index).wait_recv()
            return carry

        lax.fori_loop(0, sends, body, 0)
        turn(got.at[0], lhs2, third_offset)

    def product(edge, step, local, left):
        start = pl.multiple_of(step * STEP_ROWS, STEP_ROWS)
        right = got[edge, :, pl.ds(start, STEP_ROWS), :].reshape(2 * STEP_ROWS, width)
        for part in range(bands // half):
            columns = slice(part * half, (part + 1) * half)
            with_re = lax.dot_general(
                right, left[0, columns, :], NT, preferred_element_type=jnp.float32
            )
            with_im = lax.dot_general(
                right, left[1, columns, :], NT, preferred_element_type=jnp.float32
            )
            real = with_re[:STEP_ROWS] + with_im[STEP_ROWS:]
            imag = with_re[STEP_ROWS:] - with_im[:STEP_ROWS]
            norms = real * real + imag * imag
            squares[edge, :, :half] += norms.reshape(STEP_ROWS // 8, 8, half).sum(axis=0)
            row = lax.broadcasted_iota(jnp.int32, (STEP_ROWS, half), 0)
            column_id = lax.broadcasted_iota(jnp.int32, (STEP_ROWS, half), 1)
            on = column_id == row + (start - part * half)
            imag = jnp.where(local, with_im[:STEP_ROWS] - with_re[STEP_ROWS:], imag)
            dre[edge : edge + 1, columns] += jnp.sum(
                jnp.where(on, real, 0.0), axis=0, keepdims=True
            )
            dim[edge : edge + 1, columns] += jnp.sum(
                jnp.where(on, imag, 0.0), axis=0, keepdims=True
            )

    def trip(step, carry):
        @pl.when(step < steps)
        def _():
            @pl.when(active)
            def _():
                for inner in range(per_step):
                    index = step * per_step + inner
                    arrived(0, index).wait_recv()
                    to_cross(index).start()
                    to_along(index).start()

            product(0, step, first_local, own)

        @pl.when(step >= 1)
        def _():
            late = step - 1
            for inner in range(per_step):
                arrived(1, late * per_step + inner).wait_recv()
            product(1, late, second_local, lhs1)
            for inner in range(per_step):
                arrived(2, late * per_step + inner).wait_recv()
            product(2, late, third_local, lhs2)

        return carry

    lax.fori_loop(0, steps + 1, trip, 0)

    lane = lax.broadcasted_iota(jnp.int32, (1, bands), 1)
    found = jnp.zeros((1, bands), jnp.float32)
    for edge in range(3):
        total = jnp.sum(squares[edge], keepdims=True) / bands
        found = jnp.where(lane == 3 * slot + edge, total, found)
    phases = lax.atan2(dim[...], dre[...])
    plane[slot, 0:3, :] = phases[0:3]
    plane[slot, 6:7, :] = found

    def exchange(buffer, me, count, place, send, receive):
        copies = []
        for step in range(1, count):
            copies.append(
                pltpu.make_async_remote_copy(
                    src_ref=buffer.at[me],
                    dst_ref=buffer.at[me],
                    send_sem=send.at[step],
                    recv_sem=receive.at[me],
                    device_id=place((me + step) % count),
                    device_id_type=pl.DeviceIdType.MESH,
                )
            )
        for copy in copies:
            copy.start()
        for step in range(1, count):
            source = (me + step) % count
            pltpu.make_async_remote_copy(
                src_ref=buffer.at[source],
                dst_ref=buffer.at[source],
                send_sem=send.at[step],
                recv_sem=receive.at[source],
                device_id=place(source),
                device_id_type=pl.DeviceIdType.MESH,
            ).wait_recv()
        return copies

    copies = exchange(plane, slot, 8, in_plane, plane_send, plane_recv)
    groups = [[], [], []]
    for index in range(8):
        if index // 4 == index % 2:
            groups[0] += [plane[index, 0:1, :], plane[index, 1:2, :]]
            groups[1] += [plane[index, 2:3, :]]
        else:
            groups[1] += [plane[index, 0:1, :]]
            groups[2] += [plane[index, 1:2, :], plane[index, 2:3, :]]
    for direction in range(3):
        mean = sum(groups[direction]) / 8.0
        spreads = sum((value - mean) * (value - mean) for value in groups[direction])
        column[kz, direction : direction + 1, :] = mean
        column[kz, 3 + direction : 4 + direction, :] = spreads
    plane_found = sum(plane[index, 6:7, :] for index in range(8))
    column[kz, 6:7, :] = plane_found

    copies += exchange(column, kz, nz, in_column, column_send, column_recv)

    def merged(buffer, count, weight):
        mean = sum(buffer[index, 0:3, :] for index in range(count)) / float(count)
        spreads = sum(buffer[index, 3:6, :] for index in range(count))
        for index in range(count):
            off = buffer[index, 0:3, :] - mean
            spreads = spreads + weight * (off * off)
        return mean, spreads

    mean, spreads = merged(column, nz, 8.0)
    line[level, 0:3, :] = mean
    line[level, 3:6, :] = spreads
    line[level, 6:7, :] = plane_found
    copies += exchange(line, level, levels, in_line, line_send, line_recv)
    mean, spreads = merged(line, levels, 8.0 * nz)

    which = lax.broadcasted_iota(jnp.int32, (3, bands), 0)
    count = jnp.where(which == 0, float(nx), jnp.where(which == 1, float(ny), float(nz)))
    scale = count / (2.0 * jnp.pi)
    out_ref[0:3, :] = -count * mean / (2.0 * jnp.pi)
    out_ref[3:6, :] = scale * scale * (spreads / (nx * ny * nz))

    above = column[up, 6:7, :]
    ahead = line[(level + 1) % levels, 6:7, :]
    x_from = jnp.where(xl == 0, 3 * (core * 4 + ky), 3 * (core * 4 + ky) + 1)
    x_far = jnp.logical_and(xl == 1, core == 0)
    x_row = jnp.where(x_far, ahead, plane_found)
    y_even = 3 * (xl * 4 + (ky // 2) * 2 + 1 - xl)
    y_odd = jnp.where(xl == 1, 3 * slot + 2, 3 * ((ky + 1) % ny) + 2)
    y_from = jnp.where(core == 0, y_even, y_odd)
    z_from = jnp.where(active, 3 * (xl * 4 + sibling) + 2, 3 * slot + 1)
    z_row = jnp.where(active, above, plane_found)
    for direction, (row, place) in enumerate(
        ((x_row, x_from), (plane_found, y_from), (z_row, z_from))
    ):
        value = jnp.sum(jnp.where(lane == place, row, 0.0), axis=1, keepdims=True)
        coh_ref[direction : direction + 1, :] = jnp.broadcast_to(value, (1, 128))

    for copy in copies:
        copy.wait_send()

    def finish(index, carry):
        to_first(index).wait_send()
        to_string(index).wait_send()

        @pl.when(active)
        def _():
            to_cross(index).wait_send()
            to_along(index).wait_send()

        return carry

    lax.fori_loop(0, sends, finish, 0)


def solution(mesh):
    nx, ny, nz = mesh.shape["kx"], mesh.shape["ky"], mesh.shape["kz"]
    levels = nx // 2

    def shards(coefficients, shift_blocks):
        bands, width = coefficients.shape[4], coefficients.shape[5]
        own = coefficients.reshape(2, bands, width)
        sends = bands // SEND_ROWS
        dma = pltpu.SemaphoreType.DMA
        out, coherence = pl.pallas_call(
            functools.partial(kernel, nx, ny, nz),
            out_shape=(
                jax.ShapeDtypeStruct((6, bands), jnp.float32),
                jax.ShapeDtypeStruct((3, 128), jnp.float32),
            ),
            in_specs=[
                pl.BlockSpec(memory_space=pltpu.SMEM),
                pl.BlockSpec(memory_space=pl.ANY),
            ],
            out_specs=(
                pl.BlockSpec(memory_space=pltpu.VMEM),
                pl.BlockSpec(memory_space=pltpu.VMEM),
            ),
            scratch_shapes=[
                pltpu.VMEM((2, bands, width), jnp.bfloat16),
                pltpu.VMEM((2, bands, width), jnp.bfloat16),
                pltpu.VMEM((2, bands, width), jnp.bfloat16),
                pltpu.VMEM((3, 2, bands, width), jnp.bfloat16),
                pltpu.VMEM((8, bands), jnp.float32),
                pltpu.VMEM((8, bands), jnp.float32),
                pltpu.VMEM((3, 8, min(HALF, bands)), jnp.float32),
                pltpu.VMEM((8, 8, bands), jnp.float32),
                pltpu.VMEM((nz, 8, bands), jnp.float32),
                pltpu.VMEM((levels, 8, bands), jnp.float32),
                dma(()),
                dma((sends,)), dma((sends,)), dma((sends,)), dma((sends,)),
                dma((3, sends)),
                dma((8,)), dma((8,)),
                dma((nz,)), dma((nz,)),
                dma((levels,)), dma((levels,)),
            ],
            compiler_params=pltpu.CompilerParams(
                collective_id=0,
                has_side_effects=True,
                vmem_limit_bytes=60 * 1024 * 1024,
            ),
        )(shift_blocks, own)
        return out[0:3], out[3:6], coherence[:, 0:1].reshape(3, 1, 1, 1)

    return jax.shard_map(
        shards,
        mesh=mesh,
        in_specs=(P(None, "kx", "ky", "kz", None, None), P()),
        out_specs=(P(), P(), P(None, "kx", "ky", "kz")),
        check_vma=False,
    )
```

```python
import functools

import jax
import jax.numpy as jnp
from jax import lax
from jax.experimental import pallas as pl
from jax.experimental.pallas import tpu as pltpu
from jax.sharding import PartitionSpec as P

SEND_ROWS = 16
STEP_ROWS = 64
HALF = 256
BLOCK = 128
TILE = 16
AHEAD = 12
LAST = 128
FIRST = 64
NN = (((1,), (0,)), ((), ()))
MESH = pl.DeviceIdType.MESH


def kernel(
    nx, ny, nz,
    shift_hbm, c_ref, out_ref,
    shift_ref, result, own, turned, left, got, dre, dim, squares,
    plane_a, column_a, line_a, sheet_b, line_b,
    shift_sem, own_sem, out_sem, send_a, send_y, send_fx, send_fz, recv,
    plane_send, plane_recv, column_send, column_recv, line_send, line_recv,
    sheet_send, sheet_recv,
    second_ring, third_ring,
):
    kx, ky, kz = lax.axis_index("kx"), lax.axis_index("ky"), lax.axis_index("kz")
    bands, width = c_ref.shape[1], c_ref.shape[2]
    sends = bands // SEND_ROWS
    steps = bands // STEP_ROWS
    per_step = STEP_ROWS // SEND_ROWS
    blocks = width // BLOCK
    early = bands - LAST
    levels = nx // 2
    xl, level = kx % 2, kx // 2
    core = ky % 2
    active = xl == core
    slot = xl * 4 + ky

    def device(x, y, z):
        return (x, y, z)

    def in_plane(index):
        return device(2 * level + index // 4, index % 4, kz)

    def in_column(index):
        return device(kx, ky, index)

    def in_line(index):
        return device(2 * index + xl, ky, kz)

    sibling = ky + 1 - 2 * core
    other_x = kx + 1 - 2 * xl
    up, down = (kz + 1) % nz, (kz + nz - 1) % nz

    def signal(semaphore, peers):
        for peer in peers:
            pl.semaphore_signal(semaphore, inc=1, device_id=peer, device_id_type=MESH)

    barrier = pltpu.get_barrier_semaphore()
    beside = [in_column(up), in_column(down)]
    beside += [in_line((level + 1) % levels), in_line((level + levels - 1) % levels)]
    near = beside + [device(kx, sibling, up), device(kx, sibling, down)]
    near += [in_plane((slot + step) % 8) for step in range(1, 8)]
    next_but_one = [
        in_line((level + 2) % levels), in_line((level + levels - 2) % levels)
    ]
    signal(barrier, near)
    loads = [
        pltpu.make_async_copy(c_ref.at[:, rows, :], own.at[:, rows, :], own_sem.at[index])
        for index, rows in enumerate((pl.ds(0, FIRST), pl.ds(FIRST, bands - FIRST)))
    ]
    shift_load = pltpu.make_async_copy(shift_hbm, shift_ref, shift_sem)
    for load in loads + [shift_load]:
        load.start()
    pl.semaphore_wait(barrier, len(near))

    def rows_of(index):
        return pl.ds(pl.multiple_of(index * SEND_ROWS, SEND_ROWS), SEND_ROWS)

    def remote(source, target_slot, index, send, target):
        return pltpu.make_async_remote_copy(
            src_ref=source.at[:, rows_of(index), :],
            dst_ref=got.at[target_slot, :, rows_of(index), :],
            send_sem=send.at[index],
            recv_sem=recv.at[target_slot, index],
            device_id=target,
            device_id_type=MESH,
        )

    first_x = jnp.where(active, kx, other_x)
    first_y = jnp.where(active, sibling, ky)
    string_slot = jnp.where(active, 2, 1)
    string_y = jnp.where(active, sibling, ky)
    string_z = jnp.where(active, up, down)
    cross = device(other_x, 3 - ky, kz)
    along = device((kx + jnp.where(xl == 0, 2, nx - 2)) % nx, ky, kz)

    def to_first(index):
        return remote(own, 0, index, send_a, device(first_x, first_y, kz))

    def to_string(index):
        return remote(own, string_slot, index, send_y, device(kx, string_y, string_z))

    def to_cross(index):
        return remote(got.at[0], 2, index, send_fx, cross)

    def to_along(index):
        return remote(got.at[0], 1, index, send_fz, along)

    def arrived(edge, index):
        return pltpu.make_async_remote_copy(
            src_ref=got.at[edge, :, rows_of(index), :],
            dst_ref=got.at[edge, :, rows_of(index), :],
            send_sem=send_a.at[index],
            recv_sem=recv.at[edge, index],
            device_id=cross,
            device_id_type=MESH,
        )

    def start_own(index, carry):
        to_first(index).start()
        to_string(index).start()
        return carry

    loads[0].wait()
    lax.fori_loop(0, FIRST // SEND_ROWS, start_own, 0)
    signal(second_ring, beside)
    shift_load.wait()
    dre[...] = jnp.zeros_like(dre)
    dim[...] = jnp.zeros_like(dim)
    squares[...] = jnp.zeros_like(squares)

    first_local = jnp.where(active, xl == 1, core == 1)
    second_local = jnp.logical_and(active, xl == 0)
    third_local = jnp.logical_or(jnp.logical_not(active), xl == 0)
    second_wrap = jnp.where(
        active, jnp.where(xl == 0, kx == 0, kx == nx - 1), kz == nz - 1
    )
    third_wrap = jnp.where(active, jnp.where(xl == 0, ky == 0, ky == ny - 1), kz == 0)
    chosen = active.astype(jnp.int32)
    second_shift = chosen * shift_ref[0] + (1 - chosen) * shift_ref[2]
    third_shift = chosen * shift_ref[1] + (1 - chosen) * shift_ref[2]

    def offset(shift, wrap, local):
        wrapped, kept = wrap.astype(jnp.int32), local.astype(jnp.int32)
        return wrapped * (kept * shift + (1 - kept) * (blocks - shift))

    second_offset = offset(second_shift, second_wrap, second_local)
    third_offset = offset(third_shift, third_wrap, third_local)

    def turn(source, amount, piece, pieces):
        def body(tile, carry):
            rows = pl.ds(pl.multiple_of(tile * TILE, TILE), TILE)
            value = source[:, rows, :]
            reach = 1
            while reach < blocks:
                cut = reach * BLOCK
                moved = jnp.concatenate([value[:, :, cut:], value[:, :, :cut]], axis=2)
                value = jnp.where((amount // reach) % 2 == 1, moved, value)
                reach *= 2
            turned[:, rows, :] = value
            return carry

        share = bands // TILE // pieces
        lax.fori_loop(piece * share, (piece + 1) * share, body, 0)

    def transpose(source, edge, piece, pieces):
        def body(index, carry):
            part, block = index // blocks, index % blocks
            at = pl.ds(pl.multiple_of(block * BLOCK, BLOCK), BLOCK)
            left[edge, part, at, :] = source[part, :, at].T
            return carry

        share = 2 * blocks // pieces
        lax.fori_loop(piece * share, (piece + 1) * share, body, 0)

    def pass_on(index):
        arrived(0, index).wait_recv()
        to_cross(index).start()
        to_along(index).start()

    def while_passing(first, count, work):
        def body(piece, carry):
            @pl.when(active)
            def _():
                pass_on(first + piece)

            work(piece)
            return carry

        lax.fori_loop(0, count, body, 0)

    def third_source(piece):
        @pl.when(active)
        def _():
            turn(own, third_offset, piece, 2)

        @pl.when(jnp.logical_not(active))
        def _():
            turn(got.at[0], third_offset, piece, 2)

    loads[1].wait()
    lax.fori_loop(FIRST // SEND_ROWS, sends, start_own, 0)
    transpose(own, 0, 0, 1)
    pl.semaphore_wait(second_ring, len(beside))
    signal(third_ring, beside[0:2] + next_but_one)
    while_passing(0, 2, lambda piece: turn(own, second_offset, piece, 2))
    while_passing(2, 4, lambda piece: transpose(turned, 1, piece, 4))

    @pl.when(jnp.logical_not(active))
    def _():
        def body(index, carry):
            arrived(0, index).wait_recv()
            return carry

        lax.fori_loop(0, sends, body, 0)

    while_passing(6, 2, third_source)
    while_passing(8, 4, lambda piece: transpose(turned, 2, piece, 4))

    def product(edge, step, local):
        start = pl.multiple_of(step * STEP_ROWS, STEP_ROWS)
        right = got[edge, :, pl.ds(start, STEP_ROWS), :].reshape(2 * STEP_ROWS, width)
        for part in range(bands // HALF):
            columns = slice(part * HALF, (part + 1) * HALF)
            with_re = lax.dot_general(
                right, left[edge, 0, :, columns], NN, preferred_element_type=jnp.float32
            )
            with_im = lax.dot_general(
                right, left[edge, 1, :, columns], NN, preferred_element_type=jnp.float32
            )
            real = with_re[:STEP_ROWS] + with_im[STEP_ROWS:]
            imag = with_re[STEP_ROWS:] - with_im[:STEP_ROWS]
            norms = real * real + imag * imag
            squares[edge] += norms.reshape(STEP_ROWS // 8, 8, HALF).sum(axis=0)
            row = lax.broadcasted_iota(jnp.int32, (STEP_ROWS, HALF), 0)
            column_id = lax.broadcasted_iota(jnp.int32, (STEP_ROWS, HALF), 1)
            on = column_id == row + (start - part * HALF)
            imag = jnp.where(local, with_im[:STEP_ROWS] - with_re[STEP_ROWS:], imag)
            dre[edge : edge + 1, columns] += jnp.sum(
                jnp.where(on, real, 0.0), axis=0, keepdims=True
            )
            dim[edge : edge + 1, columns] += jnp.sum(
                jnp.where(on, imag, 0.0), axis=0, keepdims=True
            )

    def copy_of(buffer, part, me, target, count, place, send, receive, step):
        return pltpu.make_async_remote_copy(
            src_ref=buffer.at[me],
            dst_ref=buffer.at[me],
            send_sem=send.at[part, step],
            recv_sem=receive.at[part, me],
            device_id=place(target),
            device_id_type=MESH,
        )

    planes = (slot, 8, in_plane, plane_send, plane_recv)
    columns_y = (kz, nz, in_column, column_send, column_recv)
    lines = (level, levels, in_line, line_send, line_recv)

    def start_exchange(buffer, part, group):
        me, count, place, send, receive = group
        for step in range(1, count):
            target = (me + step) % count
            copy_of(buffer, part, me, target, count, place, send, receive, step).start()

    def await_exchange(buffer, part, group):
        me, count, place, send, receive = group
        for step in range(1, count):
            other = (me + step) % count
            copy_of(buffer, part, other, other, count, place, send, receive, step).wait_recv()

    def drain_exchange(buffer, part, group):
        me, count, place, send, receive = group
        for step in range(1, count):
            target = (me + step) % count
            copy_of(buffer, part, me, target, count, place, send, receive, step).wait_send()

    def plane_means(plane, column):
        groups = [[], [], []]
        for index in range(8):
            rows = [plane[index, edge : edge + 1, :] for edge in range(3)]
            if index // 4 == index % 2:
                groups[0] += rows[0:2]
                groups[1] += rows[2:3]
            else:
                groups[1] += rows[0:1]
                groups[2] += rows[1:3]
        for direction in range(3):
            mean = sum(groups[direction]) / 8.0
            spreads = sum((value - mean) * (value - mean) for value in groups[direction])
            column[kz, direction : direction + 1, :] = mean
            column[kz, 3 + direction : 4 + direction, :] = spreads

    def merged(buffer, count, weight):
        mean = sum(buffer[index, 0:3, :] for index in range(count)) / float(count)
        spreads = sum(buffer[index, 3:6, :] for index in range(count))
        for index in range(count):
            off = buffer[index, 0:3, :] - mean
            spreads = spreads + weight * (off * off)
        return mean, spreads

    def column_means(column, line):
        mean, spreads = merged(column, nz, 8.0)
        line[level, 0:3, :] = mean
        line[level, 3:6, :] = spreads

    def results(line, where):
        mean, spreads = merged(line, levels, 8.0 * nz)
        which = lax.broadcasted_iota(jnp.int32, mean.shape, 0)
        count = jnp.where(
            which == 0, float(nx), jnp.where(which == 1, float(ny), float(nz))
        )
        scale = count / (2.0 * jnp.pi)
        result[0:3, where] = -count * mean / (2.0 * jnp.pi)
        result[3:6, where] = scale * scale * (spreads / (nx * ny * nz))

    def write(where, index):
        return pltpu.make_async_copy(
            result.at[:, where], out_ref.at[:, where], out_sem.at[index]
        )

    def sheet_copy(plane_at, y_at, place, step):
        return pltpu.make_async_remote_copy(
            src_ref=sheet_b.at[y_at, plane_at],
            dst_ref=sheet_b.at[y_at, plane_at],
            send_sem=sheet_send.at[step],
            recv_sem=sheet_recv.at[y_at, plane_at],
            device_id=place,
            device_id_type=MESH,
        )

    def sheet_peers():
        for shift in range(nz):
            for step in range(8):
                if shift or step:
                    to_plane, to_y = (slot + step) % 8, (kz + shift) % nz
                    place = device(2 * level + to_plane // 4, to_plane % 4, to_y)
                    yield shift * 8 + step, to_plane, to_y, place

    def sheet_means():
        parts = [[], []]
        for y_at in range(nz):
            for index in range(8):
                parts[index // 4 != index % 2].append(sheet_b[y_at, index, 0:3, :])
        number = float(8 * nz)
        one, two = sum(parts[0]), sum(parts[1])
        means = [
            (one[0:1] + one[1:2]) / number,
            (one[2:3] + two[0:1]) / number,
            (two[1:2] + two[2:3]) / number,
        ]
        centre_one = jnp.concatenate([means[0], means[0], means[1]], axis=0)
        centre_two = jnp.concatenate([means[1], means[2], means[2]], axis=0)
        one = sum((value - centre_one) * (value - centre_one) for value in parts[0])
        two = sum((value - centre_two) * (value - centre_two) for value in parts[1])
        line_b[level, 0:3, :] = jnp.concatenate(means, axis=0)
        line_b[level, 3:4, :] = one[0:1] + one[1:2]
        line_b[level, 4:5, :] = one[2:3] + two[0:1]
        line_b[level, 5:6, :] = two[1:2] + two[2:3]

    def finish_rows(edge, step, local):
        for inner in range(per_step):
            arrived(edge, step * per_step + inner).wait_recv()
        product(edge, step, local)

    def trip(step, carry):
        few = step < 4

        def maybe_pass(place):
            index = jnp.where(
                few, AHEAD + 2 * step + place // 2, AHEAD + 8 + 4 * (step - 4) + place
            )
            due = jnp.logical_or(
                jnp.logical_and(few, place % 2 == 0),
                jnp.logical_and(jnp.logical_not(few), step < steps - 1),
            )

            @pl.when(jnp.logical_and(active, due))
            def _():
                pass_on(index)

        def follow(edge, local):
            @pl.when(step >= 1)
            def _():
                finish_rows(edge, step - 1, local)

        @pl.when(step == steps - 1)
        def _():
            phases = lax.atan2(dim[:, 0:early], dre[:, 0:early])
            plane_a[slot, 0:3, :] = phases[0:3]
            start_exchange(plane_a, 0, planes)

        maybe_pass(0)
        product(0, step, first_local)
        maybe_pass(1)
        follow(1, second_local)
        maybe_pass(2)
        follow(2, third_local)
        maybe_pass(3)
        return carry

    lax.fori_loop(0, steps, trip, 0)
    finish_rows(1, steps - 1, second_local)
    finish_rows(2, steps - 1, third_local)

    lane = lax.broadcasted_iota(jnp.int32, (1, LAST), 1)
    found = jnp.zeros((1, LAST), jnp.float32)
    for edge in range(3):
        total = jnp.sum(squares[edge], keepdims=True) / bands
        found = jnp.where(lane == 3 * slot + edge, total, found)
    phases = lax.atan2(dim[:, early:bands], dre[:, early:bands])
    sheet_b[kz, slot, 0:3, :] = phases[0:3]
    sheet_b[kz, slot, 3:4, :] = found
    pl.semaphore_wait(third_ring, 2 + len(next_but_one))
    for step, _, _, place in sheet_peers():
        sheet_copy(slot, kz, place, step).start()

    await_exchange(plane_a, 0, planes)
    plane_means(plane_a, column_a)
    start_exchange(column_a, 0, columns_y)

    for step, from_plane, from_y, place in sheet_peers():
        sheet_copy(from_plane, from_y, place, step).wait_recv()
    sheet_means()
    plane_found = sum(sheet_b[kz, index, 3:4, :] for index in range(8))
    above = sum(sheet_b[up, index, 3:4, :] for index in range(8))
    line_b[level, 6:7, :] = plane_found
    start_exchange(line_b, 1, lines)

    await_exchange(column_a, 0, columns_y)
    column_means(column_a, line_a)
    start_exchange(line_a, 0, lines)
    drain_exchange(plane_a, 0, planes)
    drain_exchange(column_a, 0, columns_y)
    for step, _, _, place in sheet_peers():
        sheet_copy(slot, kz, place, step).wait_send()

    def finish(index, carry):
        to_first(index).wait_send()
        to_string(index).wait_send()

        @pl.when(active)
        def _():
            to_cross(index).wait_send()
            to_along(index).wait_send()

        return carry

    lax.fori_loop(0, sends, finish, 0)

    await_exchange(line_b, 1, lines)
    results(line_b, slice(early, bands))
    ahead = line_b[(level + 1) % levels, 6:7, :]
    x_from = jnp.where(xl == 0, 3 * (core * 4 + ky), 3 * (core * 4 + ky) + 1)
    x_far = jnp.logical_and(xl == 1, core == 0)
    x_row = jnp.where(x_far, ahead, plane_found)
    y_even = 3 * (xl * 4 + (ky // 2) * 2 + 1 - xl)
    y_odd = jnp.where(xl == 1, 3 * slot + 2, 3 * ((ky + 1) % ny) + 2)
    y_from = jnp.where(core == 0, y_even, y_odd)
    z_from = jnp.where(active, 3 * (xl * 4 + sibling) + 2, 3 * slot + 1)
    z_row = jnp.where(active, above, plane_found)
    coherences = jnp.zeros((1, LAST), jnp.float32)
    for direction, (row, place) in enumerate(
        ((x_row, x_from), (plane_found, y_from), (z_row, z_from))
    ):
        value = jnp.sum(jnp.where(lane == place, row, 0.0), axis=1, keepdims=True)
        coherences = jnp.where(lane == direction, value, coherences)
    result[6:7, early:bands] = coherences
    write(pl.ds(early, LAST), 1).start()
    await_exchange(line_a, 0, lines)
    results(line_a, slice(0, early))
    write(pl.ds(0, early), 0).start()
    drain_exchange(line_a, 0, lines)
    drain_exchange(line_b, 1, lines)
    write(pl.ds(0, early), 0).wait()
    write(pl.ds(early, LAST), 1).wait()


def hand_out(early, found_ref, centre_ref, spread_ref, coh_ref):
    centre_ref[...] = found_ref[0:3, :]
    spread_ref[...] = found_ref[3:6, :]
    row = found_ref[6:7, early : early + LAST]
    lane = lax.broadcasted_iota(jnp.int32, (1, LAST), 1)
    for direction in range(3):
        coh_ref[direction] = jnp.sum(jnp.where(lane == direction, row, 0.0))


def solution(mesh):
    nx, ny, nz = mesh.shape["kx"], mesh.shape["ky"], mesh.shape["kz"]
    levels = nx // 2

    def shards(coefficients, shift_blocks):
        bands, width = coefficients.shape[4], coefficients.shape[5]
        own = coefficients.reshape(2, bands, width)
        sends = bands // SEND_ROWS
        dma = pltpu.SemaphoreType.DMA
        early = bands - LAST
        f32 = jnp.float32
        found = pl.pallas_call(
            functools.partial(kernel, nx, ny, nz),
            out_shape=jax.ShapeDtypeStruct((8, bands), f32),
            in_specs=[
                pl.BlockSpec(memory_space=pl.ANY),
                pl.BlockSpec(memory_space=pl.ANY),
            ],
            out_specs=pl.BlockSpec(memory_space=pl.ANY),
            scratch_shapes=[
                pltpu.SMEM((3,), jnp.int32),
                pltpu.VMEM((8, bands), f32),
                pltpu.VMEM((2, bands, width), jnp.bfloat16),
                pltpu.VMEM((2, bands, width), jnp.bfloat16),
                pltpu.VMEM((3, 2, width, bands), jnp.bfloat16),
                pltpu.VMEM((3, 2, bands, width), jnp.bfloat16),
                pltpu.VMEM((8, bands), f32),
                pltpu.VMEM((8, bands), f32),
                pltpu.VMEM((3, 8, HALF), f32),
                pltpu.VMEM((8, 4, early), f32),
                pltpu.VMEM((nz, 8, early), f32),
                pltpu.VMEM((levels, 8, early), f32),
                pltpu.VMEM((nz, 8, 4, LAST), f32),
                pltpu.VMEM((levels, 8, LAST), f32),
                dma(()), dma((2,)), dma((2,)),
                dma((sends,)), dma((sends,)), dma((sends,)), dma((sends,)),
                dma((3, sends)),
                dma((1, 8)), dma((1, 8)),
                dma((1, nz)), dma((1, nz)),
                dma((2, levels)), dma((2, levels)),
                dma((8 * nz,)), dma((nz, 8)),
                pltpu.SemaphoreType.REGULAR, pltpu.SemaphoreType.REGULAR,
            ],
            compiler_params=pltpu.CompilerParams(
                collective_id=0,
                has_side_effects=True,
                vmem_limit_bytes=60 * 1024 * 1024,
            ),
        )(shift_blocks, own)
        centre, spread, coherence = pl.pallas_call(
            functools.partial(hand_out, early),
            out_shape=(
                jax.ShapeDtypeStruct((3, bands), f32),
                jax.ShapeDtypeStruct((3, bands), f32),
                jax.ShapeDtypeStruct((3,), f32),
            ),
            out_specs=(
                pl.BlockSpec(memory_space=pltpu.VMEM),
                pl.BlockSpec(memory_space=pltpu.VMEM),
                pl.BlockSpec(memory_space=pltpu.SMEM),
            ),
        )(found)
        return centre, spread, coherence.reshape(3, 1, 1, 1)

    return jax.shard_map(
        shards,
        mesh=mesh,
        in_specs=(P(None, "kx", "ky", "kz", None, None), P()),
        out_specs=(P(), P(), P(None, "kx", "ky", "kz")),
        check_vma=False,
    )
```

```python
import functools

import jax
import jax.numpy as jnp
from jax import lax
from jax.experimental import pallas as pl
from jax.experimental.pallas import tpu as pltpu
from jax.sharding import PartitionSpec as P

SEND_ROWS = 16
STEP_ROWS = 64
HALF = 256
BLOCK = 128
TILE = 16
AHEAD = 12
LAST = 128
FIRST = 64
NN = (((1,), (0,)), ((), ()))
MESH = pl.DeviceIdType.MESH


def kernel(
    nx, ny, nz,
    shift_hbm, c_ref, result,
    shift_ref, own, turned, left, got, dre, dim, squares,
    plane_a, column_a, line_a, sheet_b, line_b,
    shift_sem, own_sem, send_a, send_y, send_fx, send_fz, first_recv, later_recv,
    group_sems,
    second_ring, third_ring,
):
    kx, ky, kz = lax.axis_index("kx"), lax.axis_index("ky"), lax.axis_index("kz")
    bands, width = c_ref.shape[1], c_ref.shape[2]
    sends = bands // SEND_ROWS
    steps = bands // STEP_ROWS
    per_step = STEP_ROWS // SEND_ROWS
    blocks = width // BLOCK
    early = bands - LAST
    levels = nx // 2
    xl, level = kx % 2, kx // 2
    core = ky % 2
    active = xl == core
    slot = xl * 4 + ky

    def device(x, y, z):
        return (x, y, z)

    def in_plane(index):
        return device(2 * level + index // 4, index % 4, kz)

    def in_column(index):
        return device(kx, ky, index)

    def in_line(index):
        return device(2 * index + xl, ky, kz)

    sibling = ky + 1 - 2 * core
    other_x = kx + 1 - 2 * xl
    up, down = (kz + 1) % nz, (kz + nz - 1) % nz

    def signal(semaphore, peers):
        for peer in peers:
            pl.semaphore_signal(semaphore, inc=1, device_id=peer, device_id_type=MESH)

    barrier = pltpu.get_barrier_semaphore()
    beside = [in_column(up), in_column(down)]
    beside += [in_line((level + 1) % levels), in_line((level + levels - 1) % levels)]
    near = beside + [device(kx, sibling, up), device(kx, sibling, down)]
    near += [in_plane((slot + step) % 8) for step in range(1, 8)]
    next_but_one = [
        in_line((level + 2) % levels), in_line((level + levels - 2) % levels)
    ]
    signal(barrier, near)
    loads = [
        pltpu.make_async_copy(c_ref.at[:, rows, :], own.at[:, rows, :], own_sem.at[index])
        for index, rows in enumerate((pl.ds(0, FIRST), pl.ds(FIRST, bands - FIRST)))
    ]
    shift_load = pltpu.make_async_copy(shift_hbm, shift_ref, shift_sem)
    for load in loads + [shift_load]:
        load.start()
    pl.semaphore_wait(barrier, len(near))

    def rows_of(index):
        return pl.ds(pl.multiple_of(index * SEND_ROWS, SEND_ROWS), SEND_ROWS)

    def remote(source, target_slot, rows, send, receive, target):
        return pltpu.make_async_remote_copy(
            src_ref=source.at[:, rows, :],
            dst_ref=got.at[target_slot, :, rows, :],
            send_sem=send,
            recv_sem=receive,
            device_id=target,
            device_id_type=MESH,
        )

    first_x = jnp.where(active, kx, other_x)
    first_y = jnp.where(active, sibling, ky)
    string_slot = jnp.where(active, 2, 1)
    string_y = jnp.where(active, sibling, ky)
    string_z = jnp.where(active, up, down)
    cross = device(other_x, 3 - ky, kz)
    along = device((kx + jnp.where(xl == 0, 2, nx - 2)) % nx, ky, kz)

    first = device(first_x, first_y, kz)
    string = device(kx, string_y, string_z)

    def to_first(index):
        return remote(own, 0, rows_of(index), send_a, first_recv.at[index], first)

    def to_string(index):
        receive = later_recv.at[string_slot - 1, index // per_step]
        return remote(own, string_slot, rows_of(index), send_y, receive, string)

    def to_cross(index):
        receive = later_recv.at[1, index // per_step]
        return remote(got.at[0], 2, rows_of(index), send_fx, receive, cross)

    def to_along(index):
        receive = later_recv.at[0, index // per_step]
        return remote(got.at[0], 1, rows_of(index), send_fz, receive, along)

    def arrived(index):
        return remote(
            got.at[0], 0, rows_of(index), send_a, first_recv.at[index], first
        )

    def step_arrived(edge, step):
        rows = pl.ds(pl.multiple_of(step * STEP_ROWS, STEP_ROWS), STEP_ROWS)
        return remote(
            got.at[0], edge, rows, send_a, later_recv.at[edge - 1, step], first
        )

    def start_own(index, carry):
        to_first(index).start()
        to_string(index).start()
        return carry

    loads[0].wait()
    lax.fori_loop(0, FIRST // SEND_ROWS, start_own, 0)
    signal(second_ring, beside)
    shift_load.wait()
    dre[...] = jnp.zeros_like(dre)
    dim[...] = jnp.zeros_like(dim)
    squares[...] = jnp.zeros_like(squares)

    first_local = jnp.where(active, xl == 1, core == 1)
    second_local = jnp.logical_and(active, xl == 0)
    third_local = jnp.logical_or(jnp.logical_not(active), xl == 0)
    second_wrap = jnp.where(
        active, jnp.where(xl == 0, kx == 0, kx == nx - 1), kz == nz - 1
    )
    third_wrap = jnp.where(active, jnp.where(xl == 0, ky == 0, ky == ny - 1), kz == 0)
    chosen = active.astype(jnp.int32)
    second_shift = chosen * shift_ref[0] + (1 - chosen) * shift_ref[2]
    third_shift = chosen * shift_ref[1] + (1 - chosen) * shift_ref[2]

    def offset(shift, wrap, local):
        wrapped, kept = wrap.astype(jnp.int32), local.astype(jnp.int32)
        return wrapped * (kept * shift + (1 - kept) * (blocks - shift))

    second_offset = offset(second_shift, second_wrap, second_local)
    third_offset = offset(third_shift, third_wrap, third_local)

    def turn(source, amount, piece, pieces):
        def body(tile, carry):
            rows = pl.ds(pl.multiple_of(tile * TILE, TILE), TILE)
            value = source[:, rows, :]
            reach = 1
            while reach < blocks:
                cut = reach * BLOCK
                moved = jnp.concatenate([value[:, :, cut:], value[:, :, :cut]], axis=2)
                value = jnp.where((amount // reach) % 2 == 1, moved, value)
                reach *= 2
            turned[:, rows, :] = value
            return carry

        share = bands // TILE // pieces
        lax.fori_loop(piece * share, (piece + 1) * share, body, 0)

    def transpose(source, edge, piece, pieces):
        def body(index, carry):
            part, block = index // blocks, index % blocks
            at = pl.ds(pl.multiple_of(block * BLOCK, BLOCK), BLOCK)
            left[edge, part, at, :] = source[part, :, at].T
            return carry

        share = 2 * blocks // pieces
        lax.fori_loop(piece * share, (piece + 1) * share, body, 0)

    def pass_on(index):
        arrived(index).wait_recv()
        to_cross(index).start()
        to_along(index).start()

    def while_passing(first, count, work):
        def body(piece, carry):
            @pl.when(active)
            def _():
                pass_on(first + piece)

            work(piece)
            return carry

        lax.fori_loop(0, count, body, 0)

    def third_source(piece):
        @pl.when(active)
        def _():
            turn(own, third_offset, piece, 2)

        @pl.when(jnp.logical_not(active))
        def _():
            turn(got.at[0], third_offset, piece, 2)

    loads[1].wait()
    lax.fori_loop(FIRST // SEND_ROWS, sends, start_own, 0)
    transpose(own, 0, 0, 1)
    pl.semaphore_wait(second_ring, len(beside))
    signal(third_ring, beside[0:2] + next_but_one)
    while_passing(0, 2, lambda piece: turn(own, second_offset, piece, 2))
    while_passing(2, 4, lambda piece: transpose(turned, 1, piece, 4))

    @pl.when(jnp.logical_not(active))
    def _():
        def body(index, carry):
            arrived(index).wait_recv()
            return carry

        lax.fori_loop(0, sends, body, 0)

    while_passing(6, 2, third_source)
    while_passing(8, 4, lambda piece: transpose(turned, 2, piece, 4))

    def product(edge, step, local):
        start = pl.multiple_of(step * STEP_ROWS, STEP_ROWS)
        right = got[edge, :, pl.ds(start, STEP_ROWS), :].reshape(2 * STEP_ROWS, width)
        for part in range(bands // HALF):
            columns = slice(part * HALF, (part + 1) * HALF)
            with_re = lax.dot_general(
                right, left[edge, 0, :, columns], NN, preferred_element_type=jnp.float32
            )
            with_im = lax.dot_general(
                right, left[edge, 1, :, columns], NN, preferred_element_type=jnp.float32
            )
            real = with_re[:STEP_ROWS] + with_im[STEP_ROWS:]
            imag = with_re[STEP_ROWS:] - with_im[:STEP_ROWS]
            norms = real * real + imag * imag
            squares[edge] += norms.reshape(STEP_ROWS // 8, 8, HALF).sum(axis=0)
            row = lax.broadcasted_iota(jnp.int32, (STEP_ROWS, HALF), 0)
            column_id = lax.broadcasted_iota(jnp.int32, (STEP_ROWS, HALF), 1)
            on = column_id == row + (start - part * HALF)
            imag = jnp.where(local, with_im[:STEP_ROWS] - with_re[STEP_ROWS:], imag)
            dre[edge : edge + 1, columns] += jnp.sum(
                jnp.where(on, real, 0.0), axis=0, keepdims=True
            )
            dim[edge : edge + 1, columns] += jnp.sum(
                jnp.where(on, imag, 0.0), axis=0, keepdims=True
            )

    def copy_of(buffer, where, target, send, receive):
        return pltpu.make_async_remote_copy(
            src_ref=buffer.at[where],
            dst_ref=buffer.at[where],
            send_sem=send,
            recv_sem=receive,
            device_id=target,
            device_id_type=MESH,
        )

    def all_of(buffer, count, send, receive):
        return copy_of(buffer, pl.ds(0, count - 1), first, send, receive)

    plane_sems, column_sems, line_a_sems, line_b_sems, sheet_sems = (
        (group_sems.at[0, index], group_sems.at[1, index]) for index in range(5)
    )
    planes = (slot, 8, in_plane)
    columns_y = (kz, nz, in_column)
    lines = (level, levels, in_line)

    def start_exchange(buffer, group, semaphores):
        me, count, place = group
        for step in range(1, count):
            copy_of(buffer, me, place((me + step) % count), *semaphores).start()

    def await_exchange(buffer, group, semaphores):
        all_of(buffer, group[1], *semaphores).wait_recv()

    def drain_exchange(buffer, group, semaphores):
        all_of(buffer, group[1], *semaphores).wait_send()

    def plane_means(plane, column):
        groups = [[], [], []]
        for index in range(8):
            rows = [plane[index, edge : edge + 1, :] for edge in range(3)]
            if index // 4 == index % 2:
                groups[0] += rows[0:2]
                groups[1] += rows[2:3]
            else:
                groups[1] += rows[0:1]
                groups[2] += rows[1:3]
        for direction in range(3):
            mean = sum(groups[direction]) / 8.0
            spreads = sum((value - mean) * (value - mean) for value in groups[direction])
            column[kz, direction : direction + 1, :] = mean
            column[kz, 3 + direction : 4 + direction, :] = spreads

    def merged(buffer, count, weight):
        mean = sum(buffer[index, 0:3, :] for index in range(count)) / float(count)
        spreads = sum(buffer[index, 3:6, :] for index in range(count))
        for index in range(count):
            off = buffer[index, 0:3, :] - mean
            spreads = spreads + weight * (off * off)
        return mean, spreads

    def column_means(column, line):
        mean, spreads = merged(column, nz, 8.0)
        line[level, 0:3, :] = mean
        line[level, 3:6, :] = spreads

    def results(line, where):
        mean, spreads = merged(line, levels, 8.0 * nz)
        which = lax.broadcasted_iota(jnp.int32, mean.shape, 0)
        count = jnp.where(
            which == 0, float(nx), jnp.where(which == 1, float(ny), float(nz))
        )
        scale = count / (2.0 * jnp.pi)
        result[0:3, where] = -count * mean / (2.0 * jnp.pi)
        result[3:6, where] = scale * scale * (spreads / (nx * ny * nz))

    def sheet_peers():
        for shift in range(nz):
            for step in range(8):
                if shift or step:
                    to_plane, to_y = (slot + step) % 8, (kz + shift) % nz
                    place = device(2 * level + to_plane // 4, to_plane % 4, to_y)
                    yield place

    def sheet_means():
        parts = [[], []]
        for y_at in range(nz):
            for index in range(8):
                parts[index // 4 != index % 2].append(sheet_b[y_at * 8 + index, 0:3, :])
        number = float(8 * nz)
        one, two = sum(parts[0]), sum(parts[1])
        means = [
            (one[0:1] + one[1:2]) / number,
            (one[2:3] + two[0:1]) / number,
            (two[1:2] + two[2:3]) / number,
        ]
        centre_one = jnp.concatenate([means[0], means[0], means[1]], axis=0)
        centre_two = jnp.concatenate([means[1], means[2], means[2]], axis=0)
        one = sum((value - centre_one) * (value - centre_one) for value in parts[0])
        two = sum((value - centre_two) * (value - centre_two) for value in parts[1])
        line_b[level, 0:3, :] = jnp.concatenate(means, axis=0)
        line_b[level, 3:4, :] = one[0:1] + one[1:2]
        line_b[level, 4:5, :] = one[2:3] + two[0:1]
        line_b[level, 5:6, :] = two[1:2] + two[2:3]

    def finish_rows(edge, step, local):
        step_arrived(edge, step).wait_recv()
        product(edge, step, local)

    def trip(step, carry):
        few = step < 4

        def maybe_pass(place):
            index = jnp.where(
                few, AHEAD + 2 * step + place // 2, AHEAD + 8 + 4 * (step - 4) + place
            )
            due = jnp.logical_or(
                jnp.logical_and(few, place % 2 == 0),
                jnp.logical_and(jnp.logical_not(few), step < steps - 1),
            )

            @pl.when(jnp.logical_and(active, due))
            def _():
                pass_on(index)

        def follow(edge, local):
            @pl.when(step >= 1)
            def _():
                finish_rows(edge, step - 1, local)

        @pl.when(step == steps - 1)
        def _():
            phases = lax.atan2(dim[:, 0:early], dre[:, 0:early])
            plane_a[slot, 0:3, :] = phases[0:3]
            start_exchange(plane_a, planes, plane_sems)

        maybe_pass(0)
        product(0, step, first_local)
        maybe_pass(1)
        follow(1, second_local)
        maybe_pass(2)
        follow(2, third_local)
        maybe_pass(3)
        return carry

    lax.fori_loop(0, steps, trip, 0)
    finish_rows(1, steps - 1, second_local)
    finish_rows(2, steps - 1, third_local)

    lane = lax.broadcasted_iota(jnp.int32, (1, LAST), 1)
    found = jnp.zeros((1, LAST), jnp.float32)
    for edge in range(3):
        total = jnp.sum(squares[edge], keepdims=True) / bands
        found = jnp.where(lane == 3 * slot + edge, total, found)
    phases = lax.atan2(dim[:, early:bands], dre[:, early:bands])
    sheet_b[kz * 8 + slot, 0:3, :] = phases[0:3]
    sheet_b[kz * 8 + slot, 3:4, :] = found
    pl.semaphore_wait(third_ring, 2 + len(next_but_one))
    for place in sheet_peers():
        copy_of(sheet_b, kz * 8 + slot, place, *sheet_sems).start()

    await_exchange(plane_a, planes, plane_sems)
    plane_means(plane_a, column_a)
    start_exchange(column_a, columns_y, column_sems)

    all_of(sheet_b, 8 * nz, *sheet_sems).wait_recv()
    sheet_means()
    plane_found = sum(sheet_b[kz * 8 + index, 3:4, :] for index in range(8))
    above = sum(sheet_b[up * 8 + index, 3:4, :] for index in range(8))
    line_b[level, 6:7, :] = plane_found
    start_exchange(line_b, lines, line_b_sems)

    await_exchange(column_a, columns_y, column_sems)
    column_means(column_a, line_a)
    start_exchange(line_a, lines, line_a_sems)
    drain_exchange(plane_a, planes, plane_sems)
    drain_exchange(column_a, columns_y, column_sems)
    all_of(sheet_b, 8 * nz, *sheet_sems).wait_send()

    everything = pl.ds(0, bands)
    remote(own, 0, everything, send_a, own_sem.at[0], first).wait_send()
    remote(own, string_slot, everything, send_y, own_sem.at[0], string).wait_send()

    @pl.when(active)
    def _():
        remote(got.at[0], 2, everything, send_fx, own_sem.at[0], cross).wait_send()
        remote(got.at[0], 1, everything, send_fz, own_sem.at[0], along).wait_send()

    await_exchange(line_b, lines, line_b_sems)
    results(line_b, slice(early, bands))
    ahead = line_b[(level + 1) % levels, 6:7, :]
    x_from = jnp.where(xl == 0, 3 * (core * 4 + ky), 3 * (core * 4 + ky) + 1)
    x_far = jnp.logical_and(xl == 1, core == 0)
    x_row = jnp.where(x_far, ahead, plane_found)
    y_even = 3 * (xl * 4 + (ky // 2) * 2 + 1 - xl)
    y_odd = jnp.where(xl == 1, 3 * slot + 2, 3 * ((ky + 1) % ny) + 2)
    y_from = jnp.where(core == 0, y_even, y_odd)
    z_from = jnp.where(active, 3 * (xl * 4 + sibling) + 2, 3 * slot + 1)
    z_row = jnp.where(active, above, plane_found)
    coherences = jnp.zeros((1, LAST), jnp.float32)
    for direction, (row, place) in enumerate(
        ((x_row, x_from), (plane_found, y_from), (z_row, z_from))
    ):
        value = jnp.sum(jnp.where(lane == place, row, 0.0), axis=1, keepdims=True)
        coherences = jnp.where(lane == direction, value, coherences)
    result[6:7, early:bands] = coherences
    await_exchange(line_a, lines, line_a_sems)
    results(line_a, slice(0, early))
    drain_exchange(line_a, lines, line_a_sems)
    drain_exchange(line_b, lines, line_b_sems)


def hand_out(early, found_ref, centre_ref, spread_ref, coh_ref):
    centre_ref[...] = found_ref[0:3, :]
    spread_ref[...] = found_ref[3:6, :]
    row = found_ref[6:7, early : early + LAST]
    lane = lax.broadcasted_iota(jnp.int32, (1, LAST), 1)
    for direction in range(3):
        coh_ref[direction] = jnp.sum(jnp.where(lane == direction, row, 0.0))


def solution(mesh):
    nx, ny, nz = mesh.shape["kx"], mesh.shape["ky"], mesh.shape["kz"]
    levels = nx // 2

    def shards(coefficients, shift_blocks):
        bands, width = coefficients.shape[4], coefficients.shape[5]
        own = coefficients.reshape(2, bands, width)
        sends = bands // SEND_ROWS
        dma = pltpu.SemaphoreType.DMA
        early = bands - LAST
        f32 = jnp.float32
        found = pl.pallas_call(
            functools.partial(kernel, nx, ny, nz),
            out_shape=jax.ShapeDtypeStruct((8, bands), f32),
            in_specs=[
                pl.BlockSpec(memory_space=pltpu.HBM),
                pl.BlockSpec(memory_space=pltpu.HBM),
            ],
            out_specs=pl.BlockSpec(memory_space=pltpu.VMEM),
            scratch_shapes=[
                pltpu.SMEM((3,), jnp.int32),
                pltpu.VMEM((2, bands, width), jnp.bfloat16),
                pltpu.VMEM((2, bands, width), jnp.bfloat16),
                pltpu.VMEM((3, 2, width, bands), jnp.bfloat16),
                pltpu.VMEM((3, 2, bands, width), jnp.bfloat16),
                pltpu.VMEM((8, bands), f32),
                pltpu.VMEM((8, bands), f32),
                pltpu.VMEM((3, 8, HALF), f32),
                pltpu.VMEM((8, 4, early), f32),
                pltpu.VMEM((nz, 8, early), f32),
                pltpu.VMEM((levels, 8, early), f32),
                pltpu.VMEM((8 * nz, 4, LAST), f32),
                pltpu.VMEM((levels, 8, LAST), f32),
                dma(()), dma((2,)),
                dma(()), dma(()), dma(()), dma(()),
                dma((sends,)), dma((2, bands // STEP_ROWS)),
                dma((2, 5)),
                pltpu.SemaphoreType.REGULAR, pltpu.SemaphoreType.REGULAR,
            ],
            compiler_params=pltpu.CompilerParams(
                collective_id=0,
                has_side_effects=True,
                vmem_limit_bytes=52 * 1024 * 1024,
            ),
        )(shift_blocks, own)
        centre, spread, coherence = pl.pallas_call(
            functools.partial(hand_out, early),
            out_shape=(
                jax.ShapeDtypeStruct((3, bands), f32),
                jax.ShapeDtypeStruct((3, bands), f32),
                jax.ShapeDtypeStruct((3,), f32),
            ),
            out_specs=(
                pl.BlockSpec(memory_space=pltpu.VMEM),
                pl.BlockSpec(memory_space=pltpu.VMEM),
                pl.BlockSpec(memory_space=pltpu.SMEM),
            ),
            compiler_params=pltpu.CompilerParams(vmem_limit_bytes=2 * 1024 * 1024),
        )(found)
        return centre, spread, coherence.reshape(3, 1, 1, 1)

    return jax.shard_map(
        shards,
        mesh=mesh,
        in_specs=(P(None, "kx", "ky", "kz", None, None), P()),
        out_specs=(P(), P(), P(None, "kx", "ky", "kz")),
        check_vma=False,
    )
```
